128 devices in a mesh: dp: 16 (over z, x), expert: 8 (over y, core).
Axes of the slice: x: 4, y: 4, z: 4, core: 2. Of those that a mesh axis runs over, the one named last changes fastest.
Arguments:
- tokens: bfloat16 [16384, 2048], P(('dp', 'expert')), may hold values from -6 to 6
- cotangent: bfloat16 [16384, 2048], P(('dp', 'expert')), may hold values from -6 to 6
- expert_ids: int32 [16384, 2], P(('dp', 'expert')), may hold values from 0 to 7, all different within a row; in each aligned block of 128 rows (0 to 127, 128 to 255, ...) at most 36 rows name the same one
- route_share: float32 [16384], P(('dp', 'expert')), may hold values from 0.5 to 0.95
- gate_proj: bfloat16 [8, 7168, 2048], P('expert', 'dp'), may hold values from -0.125 to 0.125
- up_proj: bfloat16 [8, 7168, 2048], P('expert', 'dp'), may hold values from -0.125 to 0.125
- down_anchor: float32 [8, 7168, 2048], P('expert', 'dp'), may hold values from -0.12 to 0.12
- down_average: float32 [8, 7168, 2048], P('expert', 'dp'), may hold values from -0.12 to 0.12
- down_moment: float32 [8, 7168, 2048], P('expert', 'dp'), may hold values from 0.002 to 0.05
Outputs:
- new_anchor: float32 [8, 7168, 2048], P('expert', 'dp')
- new_average: float32 [8, 7168, 2048], P('expert', 'dp')
- new_moment: float32 [8, 7168, 2048], P('expert', 'dp')
The draws below stay inside these ranges and needn't reach their ends.
Inputs may be any that keep to these rules, and one draw needn't show every extreme that they name: `expert_ids`: the two ids of a token differ. The rows of one device name any expert at most 36 times, and in every draw some device names some expert exactly 36 times.
All inputs are finite; a program needn't handle non-finite values.
Results may differ from the reference program's by a relative error of at most 0.0043.
Values may be sent and summed in bfloat16 or wider, within the bound.
A program may use at most 192 MiB of HBM per device.

```python
import math
import jax
import jax.numpy as jnp
import numpy as np
from jax import lax

D = 2048
FF = 7168
TOPK = 2
TOK_DEV = 128
EXPERTS = 8
CAP = 36
TOKENS = 16384
DEVICES = 128


def shard_levels(rng, extent, pieces, least, top_value):
    def one(position, blocks):
        draws = jax.random.uniform(jax.random.fold_in(jax.random.fold_in(rng, 6), position), (blocks,), jnp.float32, least / len(pieces), top_value / len(pieces))
        return jnp.repeat(jnp.exp(draws), extent[position] // blocks).reshape((-1,) + (1,) * (len(extent) - position - 1))

    gain = one(*pieces[0])
    for cut in pieces[1:]:
        gain = gain * one(*cut)
    return gain


def routed_block(key, own, number, rows, number_of, top, most, skew):
    order = jax.random.permutation(key, number_of)
    crowded, common = portions_of(number_of, rows * top, most, skew, True), portions_of(number_of, rows * top, most, skew, False)
    places = jnp.arange(number_of)

    def named(sizes, rotation):
        used = int((sizes > 0).sum())
        fixed = max(1, used // 4)
        passed = fixed + (places - fixed + rotation * (used - fixed)) % max(1, number_of - fixed)
        return jnp.zeros((number_of,), jnp.int32).at[order[jnp.where(places < fixed, places, passed)]].set(jnp.asarray(sizes, jnp.int32))

    sizes = jnp.where(number % 4 == 0, named(crowded, number // 4), named(common, number - number // 4 - 1))
    mixed = jax.random.permutation(jax.random.fold_in(own, 3), number_of)
    donor, sink = mixed[0:number_of // 2 * 2:2], mixed[1:number_of // 2 * 2:2]
    margin = jnp.minimum(sizes[donor] - 1, most - sizes[sink]) // 2
    margin = jnp.where((donor == order[0]) | (sink == order[0]) | (sizes[sink] == 0), 0, jnp.maximum(margin, 0))
    passed = jax.random.randint(jax.random.fold_in(own, 4), (number_of // 2,), 0, 1 << 20) % (margin + 1)
    sizes = sizes.at[donor].add(-passed).at[sink].add(passed)
    members = jnp.searchsorted(jnp.cumsum(sizes), jnp.arange(rows * top), side="right").astype(jnp.int32)
    listing = members.reshape(top, rows).T
    listing = listing[jax.random.permutation(jax.random.fold_in(own, 1), rows)]
    rotation = jax.random.randint(jax.random.fold_in(own, 2), (rows, 1), 0, top)
    return jnp.take_along_axis(listing, (jnp.arange(top)[None, :] + rotation) % top, axis=1)


def portions_of(number_of, total, limit, skew, full):
    portions = [(1 << 20) // math.isqrt(rank ** skew) + 1 for rank in range(1, number_of + 1)]
    largest = limit if full else min(limit, max(-(-total // number_of), total * portions[0] // sum(portions)))
    least = 1 if total - largest >= number_of - 1 else 0
    holding, surplus = [largest] + [least] * (number_of - 1), total - largest - least * (number_of - 1)
    while surplus > 0:
        candidates = [i for i in range(1, number_of) if holding[i] < largest] or [i for i in range(1, number_of) if holding[i] < limit]
        pool, left = sum([portions[i] for i in candidates]), surplus
        for i in candidates:
            extra = min(limit - holding[i], max(1, left * portions[i] // pool), surplus)
            holding[i] = holding[i] + extra
            surplus = surplus - extra
    return np.array(holding)


def noise(stream_key, shape, spread, reach, split=(), kind=jnp.bfloat16):
    entries = jax.random.normal(stream_key, shape, jnp.float32) * spread
    if len(split) > 0:
        entries = shard_levels(stream_key, shape, split, -0.22, 0.18) * entries
    return jnp.clip(entries, min=-reach, max=reach).astype(kind)


def setup_inputs(seed: int = 0) -> dict:
    streams_of = jax.random.split(jax.random.key(seed), 10)
    tokens = noise(streams_of[0], (TOKENS, D), 1.0, 6.0, ((0, 128),))
    cotangent = noise(streams_of[1], (TOKENS, D), 1.0, 6.0, ((0, 128),))
    expert_ids_keys = jax.random.split(jax.random.fold_in(streams_of[2], 1), TOKENS // TOK_DEV)
    expert_ids_turns = jax.random.permutation(jax.random.fold_in(streams_of[2], 3), TOKENS // TOK_DEV)
    expert_ids = jax.vmap(lambda own, number: routed_block(jax.random.fold_in(streams_of[2], 2), own, number, TOK_DEV, EXPERTS, TOPK, CAP, 1))(expert_ids_keys, expert_ids_turns).reshape((TOKENS, TOPK))
    route_share = jnp.clip(0.5 + 0.45 * jax.random.uniform(streams_of[3], (TOKENS,), jnp.float32) ** shard_levels(streams_of[3], (TOKENS,), ((0, 128),), -0.2, 0.2), 0.5, 0.95)
    gate_proj = noise(streams_of[4], (EXPERTS, FF, D), D ** -0.5, 0.125, ((0, 8), (1, 16)))
    up_proj = noise(streams_of[5], (EXPERTS, FF, D), D ** -0.5, 0.125, ((0, 8), (1, 16)))
    down_anchor = noise(streams_of[6], (EXPERTS, FF, D), 0.02, 0.12, ((0, 8), (1, 16)), jnp.float32)
    down_average = noise(streams_of[7], (EXPERTS, FF, D), 0.02, 0.12, ((0, 8), (1, 16)), jnp.float32)
    down_moment = jnp.clip(jnp.exp(math.log(0.05) - 3.218876 * jax.random.uniform(streams_of[8], (EXPERTS, FF, D), jnp.float32) ** shard_levels(streams_of[8], (EXPERTS, FF, D), ((0, 8), (1, 16)), -0.2, 0.2)), 0.002, 0.05)
    return {"tokens": tokens, "cotangent": cotangent, "expert_ids": expert_ids, "route_share": route_share, "gate_proj": gate_proj, "up_proj": up_proj, "down_anchor": down_anchor, "down_average": down_average, "down_moment": down_moment}


beta_one = 0.9
beta_two = 0.95
learn_rate = 0.05
decay_rate = 0.1
step_count = 4.0
epsilon = 1e-08

def reference(tokens, cotangent, expert_ids, route_share, gate_proj, up_proj, down_anchor, down_average, down_moment):
    shares = jnp.stack([route_share, 1.0 - route_share], axis=1)
    flat_ids = expert_ids.reshape(-1).astype(jnp.int32)
    flat_tok = (jnp.arange(TOKENS * TOPK, dtype=jnp.int32) // TOPK).astype(jnp.int32)
    flat_share = shares.reshape(-1)
    by_expert = jnp.argsort(flat_ids, stable=True).astype(jnp.int32)
    sorted_tok = flat_tok[by_expert]
    gated = (flat_share[by_expert][:, None] * cotangent[sorted_tok].astype(jnp.float32)).astype(jnp.bfloat16)
    rows_in = tokens[sorted_tok]
    expert_range = jnp.arange(EXPERTS, dtype=jnp.int32)
    counts = lax.optimization_barrier(jnp.sum((flat_ids[:, None] == expert_range[None, :]).astype(jnp.int32), axis=0)).astype(jnp.int32)
    starts = (jnp.cumsum(counts) - counts).astype(jnp.int32)
    window = DEVICES * CAP
    pad_rows = jnp.zeros((window, D), jnp.bfloat16)
    rows_in = jnp.concatenate([rows_in, pad_rows], 0)
    gated = jnp.concatenate([gated, pad_rows], 0)

    def one_expert(expert_number):
        begin_row = starts[expert_number]
        xrows = lax.dynamic_slice_in_dim(rows_in, begin_row, window, 0)
        drows = lax.dynamic_slice_in_dim(gated, begin_row, window, 0)
        live_rows = jnp.arange(window, dtype=jnp.int32) < counts[expert_number]
        drows = jnp.where(live_rows[:, None], drows, jnp.zeros_like(drows))
        gate_rows = lax.dynamic_index_in_dim(gate_proj, expert_number, 0, keepdims=False)
        up_rows = lax.dynamic_index_in_dim(up_proj, expert_number, 0, keepdims=False)
        gate_act = jnp.dot(xrows, gate_rows.T, preferred_element_type=jnp.float32)
        up_act = jnp.dot(xrows, up_rows.T, preferred_element_type=jnp.float32)
        hidden = (jax.nn.silu(gate_act) * up_act).astype(jnp.bfloat16)
        return jnp.dot(hidden.T, drows, preferred_element_type=jnp.float32)
    gradient = lax.map(one_expert, expert_range) * FF ** (-0.5)
    bias_two = 1.0 - beta_two ** step_count
    eval_point = (1.0 - beta_one) * down_anchor + beta_one * down_average
    second_moment = beta_two * down_moment + (1.0 - beta_two) * gradient * gradient
    update_dir = gradient / (jnp.sqrt(second_moment / bias_two) + epsilon) + decay_rate * eval_point
    new_anchor = down_anchor - learn_rate * update_dir
    new_average = (1.0 - 1.0 / step_count) * down_average + 1.0 / step_count * new_anchor
    return (new_anchor, new_average, second_moment)
```

```python
import jax
import jax.numpy as jnp
from jax import lax
from jax.sharding import PartitionSpec as P

FF = 7168
TOPK = 2

beta_one = 0.9
beta_two = 0.95
learn_rate = 0.05
decay_rate = 0.1
step_count = 4.0
epsilon = 1e-08

BOTH = ("dp", "expert")
SIDE = 4


def lines(along_x_for_even):
    groups = []
    for expert in range(8):
        along_x = (expert % 2 == 0) == along_x_for_even
        for fixed in range(SIDE):
            if along_x:
                dps = [fixed * SIDE + i for i in range(SIDE)]
            else:
                dps = [i * SIDE + fixed for i in range(SIDE)]
            groups.append([dp * 8 + expert for dp in dps])
    return groups


WEIGHT_LINES = lines(True)
ROW_LINES = lines(False)


def shards(
    tokens,
    cotangent,
    expert_ids,
    route_share,
    gate_proj,
    up_proj,
    down_anchor,
    down_average,
    down_moment,
):
    experts_all = lax.axis_size("expert")
    tok_rows = tokens.shape[0]
    width = tokens.shape[1]
    capacity = tok_rows * TOPK // experts_all * 9 // 8
    slots = experts_all * capacity
    weight_gate = lax.all_gather(gate_proj[0], BOTH, axis=0, tiled=True, axis_index_groups=WEIGHT_LINES)
    weight_up = lax.all_gather(up_proj[0], BOTH, axis=0, tiled=True, axis_index_groups=WEIGHT_LINES)
    shares = jnp.stack([route_share, 1.0 - route_share], axis=1)
    expert_range = jnp.arange(experts_all, dtype=jnp.int32)
    flat_ids = expert_ids.reshape(-1)
    onehot_routes = (flat_ids[:, None] == expert_range[None, :]).astype(jnp.int32)
    earlier = jnp.cumsum(onehot_routes, axis=0) - onehot_routes
    slot_of = jnp.sum(earlier * onehot_routes, axis=1)
    target = (flat_ids * capacity + slot_of).reshape(tok_rows, TOPK)
    slot_range = jnp.arange(slots, dtype=jnp.int32)
    placed = target[None, :, :] == slot_range[:, None, None]
    picker = jnp.sum(placed.astype(jnp.float32), axis=2).astype(jnp.bfloat16)
    slot_share = jnp.sum(jnp.where(placed, shares[None, :, :], 0.0), axis=(1, 2))
    send_rows = jnp.dot(picker, tokens, preferred_element_type=jnp.float32).astype(jnp.bfloat16)
    send_grad = (
        slot_share[:, None] * jnp.dot(picker, cotangent, preferred_element_type=jnp.float32)
    ).astype(jnp.bfloat16)
    rows_here = lax.all_to_all(
        send_rows.reshape(experts_all, capacity, width), "expert",
        split_axis=0, concat_axis=0, tiled=True,
    ).reshape(slots, width)
    grad_here = lax.all_to_all(
        send_grad.reshape(experts_all, capacity, width), "expert",
        split_axis=0, concat_axis=0, tiled=True,
    ).reshape(slots, width)
    rows_all = lax.all_gather(rows_here, BOTH, axis=0, tiled=True, axis_index_groups=ROW_LINES)
    grad_all = lax.all_gather(grad_here, BOTH, axis=0, tiled=True, axis_index_groups=ROW_LINES)
    gate_act = lax.dot_general(
        rows_all, weight_gate, (((1,), (1,)), ((), ())), preferred_element_type=jnp.float32
    )
    up_act = lax.dot_general(
        rows_all, weight_up, (((1,), (1,)), ((), ())), preferred_element_type=jnp.float32
    )
    hidden = (jax.nn.silu(gate_act) * up_act).astype(jnp.bfloat16)
    part = lax.dot_general(
        hidden, grad_all, (((0,), (0,)), ((), ())), preferred_element_type=jnp.float32
    ).astype(jnp.bfloat16)
    gradient = lax.psum_scatter(
        part, BOTH, scatter_dimension=0, tiled=True, axis_index_groups=WEIGHT_LINES
    ).astype(jnp.float32)
    gradient = gradient[None] * FF ** (-0.5)
    bias_two = 1.0 - beta_two**step_count
    eval_point = (1.0 - beta_one) * down_anchor + beta_one * down_average
    second_moment = beta_two * down_moment + (1.0 - beta_two) * gradient * gradient
    update_dir = gradient / (jnp.sqrt(second_moment / bias_two) + epsilon) + decay_rate * eval_point
    new_anchor = down_anchor - learn_rate * update_dir
    new_average = (1.0 - 1.0 / step_count) * down_average + 1.0 / step_count * new_anchor
    return (new_anchor, new_average, second_moment)


def solution(mesh):
    placed = (
        P(("dp", "expert"), None),
        P(("dp", "expert"), None),
        P(("dp", "expert"), None),
        P(("dp", "expert")),
        P("expert", "dp", None),
        P("expert", "dp", None),
        P("expert", "dp", None),
        P("expert", "dp", None),
        P("expert", "dp", None),
    )
    return jax.shard_map(
        shards,
        mesh=mesh,
        in_specs=placed,
        out_specs=(P("expert", "dp", None), P("expert", "dp", None), P("expert", "dp", None)),
        check_vma=False,
    )
```

```python
import functools

import jax
import jax.numpy as jnp
from jax import lax
from jax.experimental import pallas as pl
from jax.experimental.pallas import tpu as pltpu
from jax.sharding import PartitionSpec as P

FF = 7168
TOPK = 2

beta_one = 0.9
beta_two = 0.95
learn_rate = 0.05
decay_rate = 0.1
step_count = 4.0
epsilon = 1e-08

SIDE = 4
CHUNKS = 4
MESH = pl.DeviceIdType.MESH
NT = (((1,), (1,)), ((), ()))


def dot(a, b):
    return jnp.dot(a, b, preferred_element_type=jnp.float32)


def exchange(
    experts,
    cap,
    tok_ref,
    cot_ref,
    ids_ref,
    share_ref,
    gate_ref,
    up_ref,
    out_ref,
    pack,
    land,
    rows,
    grads,
    weights,
    hid,
    hid_t,
    part,
    opp_in,
    dir_in,
    acc_in,
    own_sem,
    w_send,
    w_recv,
    a_send,
    a_recv,
    r_send,
    r_recv,
    opp_send,
    opp_recv,
    dir_send,
    dir_recv,
    acc_send,
    acc_recv,
):
    dp = lax.axis_index("dp")
    me = lax.axis_index("expert")
    core = me % 2
    hi, lo = dp // SIDE, dp % SIDE
    p = core * hi + (1 - core) * lo
    q = core * lo + (1 - core) * hi

    def peer(p_to, q_to, e_to):
        to = core * (p_to * SIDE + q_to) + (1 - core) * (q_to * SIDE + p_to)
        return {"dp": to, "expert": e_to}

    p_left, p_right, p_far = (p + 3) % SIDE, (p + 1) % SIDE, (p + 2) % SIDE
    q_left, q_right, q_far = (q + 3) % SIDE, (q + 1) % SIDE, (q + 2) % SIDE
    w_left, w_right = peer(p_left, q, me), peer(p_right, q, me)
    r_left, r_right = peer(p, q_left, me), peer(p, q_right, me)

    barrier = pltpu.get_barrier_semaphore()
    for to in (w_left, w_right, r_left, r_right):
        pl.semaphore_signal(barrier, inc=1, device_id=to, device_id_type=MESH)
    for i in range(1, experts):
        pl.semaphore_signal(
            barrier, inc=1, device_id=peer(p, q, (me + i) % experts), device_id_type=MESH
        )
    pl.semaphore_wait(barrier, 4 + experts - 1)

    def remote(src, dst, send, recv, to):
        return pltpu.make_async_remote_copy(
            src_ref=src, dst_ref=dst, send_sem=send, recv_sem=recv, device_id=to,
            device_id_type=MESH,
        )

    def weight_copy(i):
        if i == 0:
            return remote(gate_ref, weights.at[p, 0], w_send.at[0], w_recv.at[0], w_left)
        if i == 1:
            return remote(up_ref, weights.at[p, 1], w_send.at[1], w_recv.at[1], w_right)
        if i == 2:
            return remote(up_ref, weights.at[p, 1], w_send.at[2], w_recv.at[2], w_left)
        if i == 3:
            return remote(gate_ref, weights.at[p, 0], w_send.at[3], w_recv.at[3], w_right)
        if i == 4:
            ref = weights.at[p_right, 0]
            return remote(ref, ref, w_send.at[4], w_recv.at[4], w_left)
        ref = weights.at[p_left, 1]
        return remote(ref, ref, w_send.at[5], w_recv.at[5], w_right)

    for i in range(4):
        weight_copy(i).start()
    own_gate = pltpu.make_async_copy(gate_ref, weights.at[p, 0], own_sem.at[0])
    own_up = pltpu.make_async_copy(up_ref, weights.at[p, 1], own_sem.at[1])
    own_gate.start()
    own_up.start()

    toks = tok_ref.shape[0]
    number = lax.broadcasted_iota(jnp.int32, (experts, toks), 0)
    before = (
        lax.broadcasted_iota(jnp.int32, (toks, toks), 0)
        < lax.broadcasted_iota(jnp.int32, (toks, toks), 1)
    ).astype(jnp.bfloat16)
    id_a, id_b = ids_ref[0:1, :], ids_ref[1:2, :]
    hot_a = (number == id_a).astype(jnp.float32)
    hot_b = (number == id_b).astype(jnp.float32)
    count_a = dot(hot_a.astype(jnp.bfloat16), before)
    count_b = dot(hot_b.astype(jnp.bfloat16), before) + jnp.sum(hot_a, axis=1, keepdims=True)
    slot_a = jnp.sum(hot_a * count_a, axis=0, keepdims=True).astype(jnp.int32)
    slot_b = jnp.sum(hot_b * count_b, axis=0, keepdims=True).astype(jnp.int32)
    share = share_ref[...]
    line = lax.broadcasted_iota(jnp.int32, (2 * cap, toks), 0)

    def fill(i, carry):
        to = (me + i) % experts
        at_a = jnp.where(id_a == to, slot_a, -1 - 2 * cap)
        at_b = jnp.where(id_b == to, slot_b, -1 - 2 * cap)
        row_pick = ((line == at_a) | (line == at_b)).astype(jnp.float32).astype(jnp.bfloat16)
        low_a, low_b = line == at_a + cap, line == at_b + cap
        grad_pick = (low_a | low_b).astype(jnp.float32).astype(jnp.bfloat16)
        scale = jnp.sum(
            jnp.where(low_a, share, 0.0) + jnp.where(low_b, 1.0 - share, 0.0),
            axis=1,
            keepdims=True,
        )
        both = dot(row_pick, tok_ref[...]) + scale * dot(grad_pick, cot_ref[...])
        pack[to] = both.astype(jnp.bfloat16)
        return carry

    lax.fori_loop(0, experts, fill, 0)

    def route_copy(i):
        to = (me + i) % experts
        return remote(
            pack.at[to], land.at[me], a_send.at[i - 1], a_recv.at[i - 1], peer(p, q, to)
        )

    for i in range(1, experts):
        route_copy(i).start()
    land[me] = pack[me]

    weight_copy(0).wait_recv()
    weight_copy(4).start()
    weight_copy(1).wait_recv()
    weight_copy(5).start()

    for i in range(1, experts):
        route_copy(i).wait_recv()

    block = experts * cap
    wide = lax.broadcasted_iota(jnp.int32, (block, 2 * block), 1)
    deep = lax.broadcasted_iota(jnp.int32, (block, 2 * block), 0)
    source = jnp.floor((wide.astype(jnp.float32) + 0.5) * (1.0 / (2 * cap))).astype(jnp.int32)
    inside = wide - source * (2 * cap)
    row_from = jnp.where(inside < cap, source * cap + inside, -1)
    grad_from = jnp.where(inside >= cap, source * cap + inside - cap, -1)
    landed = land[...].reshape(2 * block, land.shape[2])
    pick = (deep == row_from).astype(jnp.float32).astype(jnp.bfloat16)
    rows[q] = dot(pick, landed).astype(jnp.bfloat16)
    pick = (deep == grad_from).astype(jnp.float32).astype(jnp.bfloat16)
    grads[q] = dot(pick, landed).astype(jnp.bfloat16)

    def row_copy(i):
        if i == 0:
            return remote(rows.at[q], rows.at[q], r_send.at[0], r_recv.at[0], r_left)
        if i == 1:
            return remote(grads.at[q], grads.at[q], r_send.at[1], r_recv.at[1], r_right)
        if i == 2:
            return remote(grads.at[q], grads.at[q], r_send.at[2], r_recv.at[2], r_left)
        if i == 3:
            return remote(rows.at[q], rows.at[q], r_send.at[3], r_recv.at[3], r_right)
        if i == 4:
            ref = rows.at[q_right]
            return remote(ref, ref, r_send.at[4], r_recv.at[4], r_left)
        ref = grads.at[q_left]
        return remote(ref, ref, r_send.at[5], r_recv.at[5], r_right)

    for i in range(4):
        row_copy(i).start()

    def forward(b, s):
        x = rows[b]
        gate = lax.dot_general(x, weights[s, 0], NT, preferred_element_type=jnp.float32)
        up = lax.dot_general(x, weights[s, 1], NT, preferred_element_type=jnp.float32)
        hid[s, b] = (gate / (1.0 + jnp.exp(-gate)) * up).astype(jnp.bfloat16)

    def forward_near(b):
        def step(i, carry):
            forward(b, (p + 3 + i) % SIDE)
            return carry

        lax.fori_loop(0, 3, step, 0)

    own_gate.wait()
    own_up.wait()
    weight_copy(2).wait_recv()
    weight_copy(3).wait_recv()
    forward_near(q)
    row_copy(0).wait_recv()
    row_copy(4).start()
    row_copy(1).wait_recv()
    row_copy(5).start()
    forward_near(q_right)
    row_copy(3).wait_recv()
    forward_near(q_left)
    weight_copy(4).wait_recv()
    weight_copy(5).wait_recv()

    def step_far(i, carry):
        forward((q + 3 + i) % SIDE, p_far)
        return carry

    lax.fori_loop(0, 3, step_far, 0)
    row_copy(2).wait_recv()
    row_copy(4).wait_recv()
    row_copy(5).wait_recv()

    def far_copy(c):
        return remote(
            part.at[p_far, c], opp_in.at[c], opp_send.at[c], opp_recv.at[c],
            peer((p + 3 + 2 * (c // 2)) % SIDE, q, me),
        )

    def near_copy(c):
        to = (p + 1 + 2 * (c // 2)) % SIDE
        return remote(
            part.at[to, c], dir_in.at[c], dir_send.at[c], dir_recv.at[c], peer(to, q, me)
        )

    def sum_copy(c):
        to = (p + 3 + 2 * (c // 2)) % SIDE
        return remote(
            part.at[to, c], acc_in.at[c], acc_send.at[c], acc_recv.at[c], peer(to, q, me)
        )

    all_rows = SIDE * block
    full = hid.shape[3]
    chunk = part.shape[3]

    def backward(s, first, send):
        forward(q_far, s)
        hid_t[...] = hid[s].reshape(all_rows, full).T

        def step(j, carry):
            c = (first + j) % CHUNKS
            at = pl.ds(pl.multiple_of(c * chunk, chunk), chunk)
            grad = grads[:, :, at].reshape(all_rows, chunk)
            part[s, c] = dot(hid_t[...], grad).astype(jnp.bfloat16)
            return carry

        lax.fori_loop(0, CHUNKS, step, 0)
        for c in send:
            if s is p_far:
                far_copy(c).start()
            else:
                near_copy(c).start()

    backward(p_far, 0, (0, 2, 1, 3))
    backward(p_left, 2, (2, 3))
    backward(p_right, 0, (0, 1))
    for c in (0, 2, 1, 3):
        far_copy(c).wait_recv()
        to = (p + 3 + 2 * (c // 2)) % SIDE
        part[to, c] = (
            part[to, c].astype(jnp.float32) + opp_in[c].astype(jnp.float32)
        ).astype(jnp.bfloat16)
        sum_copy(c).start()
    backward(p, 0, ())
    for c in (0, 2, 1, 3):
        near_copy(c).wait_recv()
        sum_copy(c).wait_recv()
        out_ref[:, c * chunk : (c + 1) * chunk] = (
            part[p, c].astype(jnp.float32)
            + dir_in[c].astype(jnp.float32)
            + acc_in[c].astype(jnp.float32)
        )
    for i in range(6):
        weight_copy(i).wait_send()
        row_copy(i).wait_send()
    for i in range(1, experts):
        route_copy(i).wait_send()
    for c in range(CHUNKS):
        far_copy(c).wait_send()
        near_copy(c).wait_send()
        sum_copy(c).wait_send()


def shards(
    tokens,
    cotangent,
    expert_ids,
    route_share,
    gate_proj,
    up_proj,
    down_anchor,
    down_average,
    down_moment,
):
    experts = lax.axis_size("expert")
    toks, width = tokens.shape
    cap = toks * TOPK // experts * 9 // 8
    block = experts * cap
    full = gate_proj.shape[1]
    chunk = width // CHUNKS
    bf16 = jnp.bfloat16
    vmem = pl.BlockSpec(memory_space=pltpu.VMEM)
    hbm = pl.BlockSpec(memory_space=pl.ANY)
    dma = pltpu.SemaphoreType.DMA
    gradient = pl.pallas_call(
        functools.partial(exchange, experts, cap),
        out_shape=jax.ShapeDtypeStruct((full, width), jnp.float32),
        in_specs=[vmem, vmem, vmem, vmem, hbm, hbm],
        out_specs=vmem,
        scratch_shapes=[
            pltpu.VMEM((experts, 2 * cap, width), bf16),
            pltpu.VMEM((experts, 2 * cap, width), bf16),
            pltpu.VMEM((SIDE, block, width), bf16),
            pltpu.VMEM((SIDE, block, width), bf16),
            pltpu.VMEM((SIDE, 2, full, width), bf16),
            pltpu.VMEM((SIDE, SIDE, block, full), bf16),
            pltpu.VMEM((full, SIDE * block), bf16),
            pltpu.VMEM((SIDE, CHUNKS, full, chunk), bf16),
            pltpu.VMEM((CHUNKS, full, chunk), bf16),
            pltpu.VMEM((CHUNKS, full, chunk), bf16),
            pltpu.VMEM((CHUNKS, full, chunk), bf16),
            dma((2,)),
            dma((6,)),
            dma((6,)),
            dma((experts - 1,)),
            dma((experts - 1,)),
            dma((6,)),
            dma((6,)),
            dma((CHUNKS,)),
            dma((CHUNKS,)),
            dma((CHUNKS,)),
            dma((CHUNKS,)),
            dma((CHUNKS,)),
            dma((CHUNKS,)),
        ],
        compiler_params=pltpu.CompilerParams(
            collective_id=0, has_side_effects=True, vmem_limit_bytes=67043328
        ),
        name="exchange",
    )(tokens, cotangent, expert_ids.T, route_share[None], gate_proj[0], up_proj[0])
    gradient = gradient[None] * FF ** (-0.5)
    bias_two = 1.0 - beta_two**step_count
    eval_point = (1.0 - beta_one) * down_anchor + beta_one * down_average
    second_moment = beta_two * down_moment + (1.0 - beta_two) * gradient * gradient
    update_dir = gradient / (jnp.sqrt(second_moment / bias_two) + epsilon) + decay_rate * eval_point
    new_anchor = down_anchor - learn_rate * update_dir
    new_average = (1.0 - 1.0 / step_count) * down_average + 1.0 / step_count * new_anchor
    return (new_anchor, new_average, second_moment)


def solution(mesh):
    placed = (
        P(("dp", "expert"), None),
        P(("dp", "expert"), None),
        P(("dp", "expert"), None),
        P(("dp", "expert")),
        P("expert", "dp", None),
        P("expert", "dp", None),
        P("expert", "dp", None),
        P("expert", "dp", None),
        P("expert", "dp", None),
    )
    return jax.shard_map(
        shards,
        mesh=mesh,
        in_specs=placed,
        out_specs=(P("expert", "dp", None), P("expert", "dp", None), P("expert", "dp", None)),
        check_vma=False,
    )
```

```python
import functools

import jax
import jax.numpy as jnp
from jax import lax
from jax.experimental import pallas as pl
from jax.experimental.pallas import tpu as pltpu
from jax.sharding import PartitionSpec as P

FF = 7168
TOPK = 2

beta_one = 0.9
beta_two = 0.95
learn_rate = 0.05
decay_rate = 0.1
step_count = 4.0
epsilon = 1e-08

SIDE = 4
CHUNKS = 4
MESH = pl.DeviceIdType.MESH
NT = (((1,), (1,)), ((), ()))


def dot(a, b):
    return jnp.dot(a, b, preferred_element_type=jnp.float32)


def exchange(
    experts,
    cap,
    tok_ref,
    cot_ref,
    ids_ref,
    share_ref,
    gate_ref,
    up_ref,
    out_ref,
    pack,
    land,
    rows,
    grads,
    weights,
    hid,
    hid_t,
    part,
    opp_in,
    dir_in,
    acc_in,
    total,
    own_sem,
    w_send,
    w_recv,
    a_send,
    a_recv,
    r_send,
    r_recv,
    opp_send,
    opp_recv,
    dir_send,
    dir_recv,
    acc_send,
    acc_recv,
):
    dp = lax.axis_index("dp")
    me = lax.axis_index("expert")
    core = me % 2
    hi, lo = dp // SIDE, dp % SIDE
    p = core * hi + (1 - core) * lo
    q = core * lo + (1 - core) * hi

    def peer(p_to, q_to, e_to):
        to = core * (p_to * SIDE + q_to) + (1 - core) * (q_to * SIDE + p_to)
        return {"dp": to, "expert": e_to}

    p_left, p_right, p_far = (p + 3) % SIDE, (p + 1) % SIDE, (p + 2) % SIDE
    q_left, q_right, q_far = (q + 3) % SIDE, (q + 1) % SIDE, (q + 2) % SIDE
    w_left, w_right = peer(p_left, q, me), peer(p_right, q, me)
    r_left, r_right = peer(p, q_left, me), peer(p, q_right, me)

    barrier = pltpu.get_barrier_semaphore()
    for to in (w_left, w_right, r_left, r_right):
        pl.semaphore_signal(barrier, inc=1, device_id=to, device_id_type=MESH)
    for i in range(1, experts):
        pl.semaphore_signal(
            barrier, inc=1, device_id=peer(p, q, (me + i) % experts), device_id_type=MESH
        )

    def remote(src, dst, send, recv, to):
        return pltpu.make_async_remote_copy(
            src_ref=src, dst_ref=dst, send_sem=send, recv_sem=recv, device_id=to,
            device_id_type=MESH,
        )

    def weight_copy(i):
        if i == 0:
            return remote(gate_ref, weights.at[p, 0], w_send.at[0], w_recv.at[0], w_left)
        if i == 1:
            return remote(up_ref, weights.at[p, 1], w_send.at[1], w_recv.at[1], w_right)
        if i == 2:
            return remote(up_ref, weights.at[p, 1], w_send.at[2], w_recv.at[2], w_left)
        if i == 3:
            return remote(gate_ref, weights.at[p, 0], w_send.at[3], w_recv.at[3], w_right)
        if i == 4:
            ref = weights.at[p_right, 0]
            return remote(ref, ref, w_send.at[4], w_recv.at[4], w_left)
        ref = weights.at[p_left, 1]
        return remote(ref, ref, w_send.at[5], w_recv.at[5], w_right)

    own_gate = pltpu.make_async_copy(gate_ref, weights.at[p, 0], own_sem.at[0])
    own_up = pltpu.make_async_copy(up_ref, weights.at[p, 1], own_sem.at[1])
    own_gate.start()
    own_up.start()

    toks = tok_ref.shape[0]
    number = lax.broadcasted_iota(jnp.int32, (experts, toks), 0)
    before = (
        lax.broadcasted_iota(jnp.int32, (toks, toks), 0)
        < lax.broadcasted_iota(jnp.int32, (toks, toks), 1)
    ).astype(jnp.bfloat16)
    id_a, id_b = ids_ref[0:1, :], ids_ref[1:2, :]
    hot_a = (number == id_a).astype(jnp.float32)
    hot_b = (number == id_b).astype(jnp.float32)
    count_a = dot(hot_a.astype(jnp.bfloat16), before)
    count_b = dot(hot_b.astype(jnp.bfloat16), before) + jnp.sum(hot_a, axis=1, keepdims=True)
    slot_a = jnp.sum(hot_a * count_a, axis=0, keepdims=True).astype(jnp.int32)
    slot_b = jnp.sum(hot_b * count_b, axis=0, keepdims=True).astype(jnp.int32)
    share = share_ref[...]
    line = lax.broadcasted_iota(jnp.int32, (2 * cap, toks), 0)

    def fill(i, carry):
        to = (me + i) % experts
        at_a = jnp.where(id_a == to, slot_a, -1 - 2 * cap)
        at_b = jnp.where(id_b == to, slot_b, -1 - 2 * cap)
        row_pick = ((line == at_a) | (line == at_b)).astype(jnp.float32).astype(jnp.bfloat16)
        low_a, low_b = line == at_a + cap, line == at_b + cap
        grad_pick = (low_a | low_b).astype(jnp.float32).astype(jnp.bfloat16)
        scale = jnp.sum(
            jnp.where(low_a, share, 0.0) + jnp.where(low_b, 1.0 - share, 0.0),
            axis=1,
            keepdims=True,
        )
        both = dot(row_pick, tok_ref[...]) + scale * dot(grad_pick, cot_ref[...])
        pack[to] = both.astype(jnp.bfloat16)
        return carry

    lax.fori_loop(0, experts, fill, 0)
    pl.semaphore_wait(barrier, 4 + experts - 1)
    for i in range(4):
        weight_copy(i).start()

    def route_copy(i):
        to = (me + i) % experts
        return remote(
            pack.at[to], land.at[me], a_send.at[i - 1], a_recv.at[i - 1], peer(p, q, to)
        )

    for i in range(1, experts):
        route_copy(i).start()
    land[me] = pack[me]

    for i in range(1, experts):
        route_copy(i).wait_recv()

    block = experts * cap
    wide = lax.broadcasted_iota(jnp.int32, (block, 2 * block), 1)
    deep = lax.broadcasted_iota(jnp.int32, (block, 2 * block), 0)
    source = jnp.floor((wide.astype(jnp.float32) + 0.5) * (1.0 / (2 * cap))).astype(jnp.int32)
    inside = wide - source * (2 * cap)
    row_from = jnp.where(inside < cap, source * cap + inside, -1)
    grad_from = jnp.where(inside >= cap, source * cap + inside - cap, -1)
    landed = land[...].reshape(2 * block, land.shape[2])
    pick = (deep == row_from).astype(jnp.float32).astype(jnp.bfloat16)
    rows[q] = dot(pick, landed).astype(jnp.bfloat16)
    pick = (deep == grad_from).astype(jnp.float32).astype(jnp.bfloat16)
    grads[q] = dot(pick, landed).astype(jnp.bfloat16)

    def row_copy(i):
        if i == 0:
            return remote(rows.at[q], rows.at[q], r_send.at[0], r_recv.at[0], r_left)
        if i == 1:
            return remote(grads.at[q], grads.at[q], r_send.at[1], r_recv.at[1], r_right)
        if i == 2:
            return remote(grads.at[q], grads.at[q], r_send.at[2], r_recv.at[2], r_left)
        if i == 3:
            return remote(rows.at[q], rows.at[q], r_send.at[3], r_recv.at[3], r_right)
        half = pl.ds((i - 4) // 2 * (block // 2), block // 2)
        if i % 2 == 0:
            ref = rows.at[q_right, half]
            return remote(ref, ref, r_send.at[i], r_recv.at[i], r_left)
        ref = grads.at[q_left, half]
        return remote(ref, ref, r_send.at[i], r_recv.at[i], r_right)

    for i in range(4):
        row_copy(i).start()

    def forward(b, s):
        x = rows[b]
        gate = lax.dot_general(x, weights[s, 0], NT, preferred_element_type=jnp.float32)
        up = lax.dot_general(x, weights[s, 1], NT, preferred_element_type=jnp.float32)
        hid[s, b] = (gate / (1.0 + jnp.exp(-gate)) * up).astype(jnp.bfloat16)

    def forward_near(b):
        def step(i, carry):
            forward(b, (p + 3 + i) % SIDE)
            return carry

        lax.fori_loop(0, 3, step, 0)

    own_gate.wait()
    own_up.wait()
    for i in range(4):
        weight_copy(i).wait_recv()
    forward_near(q)
    row_copy(0).wait_recv()
    row_copy(4).start()
    row_copy(6).start()
    row_copy(1).wait_recv()
    row_copy(5).start()
    row_copy(7).start()
    forward_near(q_right)
    row_copy(3).wait_recv()
    forward_near(q_left)
    row_copy(2).wait_recv()
    row_copy(4).wait_recv()
    weight_copy(4).start()
    row_copy(5).wait_recv()
    weight_copy(5).start()
    row_copy(6).wait_recv()
    row_copy(7).wait_recv()

    def far_copy(c):
        return remote(
            part.at[1, c], opp_in.at[c], opp_send.at[c], opp_recv.at[c],
            peer((p + 3 + 2 * (c // 2)) % SIDE, q, me),
        )

    def near_copy(c):
        to = (p + 1 + 2 * (c // 2)) % SIDE
        return remote(
            part.at[2 * (c // 2), c], dir_in.at[c], dir_send.at[c], dir_recv.at[c], peer(to, q, me)
        )

    def sum_copy(c):
        to = (p + 3 + 2 * (c // 2)) % SIDE
        return remote(
            part.at[2 - 2 * (c // 2), c], acc_in.at[c], acc_send.at[c], acc_recv.at[c], peer(to, q, me)
        )

    all_rows = SIDE * block
    full = hid.shape[3]
    chunk = part.shape[3]

    def turn(s):
        hid_t[...] = hid[s].reshape(all_rows, full).T

    def backward(c):
        at = pl.ds(pl.multiple_of(c * chunk, chunk), chunk)
        return dot(hid_t[...], grads[:, :, at].reshape(all_rows, chunk))

    def near_slice(first, s, place):
        forward(q_far, s)
        turn(s)

        def step(j, carry):
            c = (first + j) % CHUNKS
            part[place, c] = backward(c).astype(jnp.bfloat16)

            @pl.when(j < 2)
            def _():
                near_copy(c).start()

            return carry

        lax.fori_loop(0, CHUNKS, step, 0)

    near_slice(2, p_left, 2)
    near_slice(0, p_right, 0)
    forward(q_far, p)
    turn(p)

    def own_step(c, carry):
        total[c] = backward(c)
        return carry

    lax.fori_loop(0, CHUNKS, own_step, 0)

    weight_copy(4).wait_recv()
    weight_copy(5).wait_recv()

    def far_forward(b, carry):
        forward(b, p_far)
        return carry

    lax.fori_loop(0, SIDE, far_forward, 0)
    turn(p_far)

    def far_step(j, carry):
        c = (j % 2) * 2 + j // 2
        part[1, c] = backward(c).astype(jnp.bfloat16)
        far_copy(c).start()
        return carry

    lax.fori_loop(0, CHUNKS, far_step, 0)

    def relay(j, carry):
        c = (j % 2) * 2 + j // 2
        far_copy(c).wait_recv()
        place = 2 - 2 * (c // 2)
        part[place, c] = (
            part[place, c].astype(jnp.float32) + opp_in[c].astype(jnp.float32)
        ).astype(jnp.bfloat16)
        sum_copy(c).start()
        return carry

    lax.fori_loop(0, CHUNKS, relay, 0)

    def result_copy(c):
        return pltpu.make_async_copy(total.at[c], out_ref.at[c], own_sem.at[2 + c])

    for c in range(CHUNKS):
        near_copy(c).wait_recv()
        total[c] = total[c] + dir_in[c].astype(jnp.float32)
    for c in (0, 2, 1, 3):
        sum_copy(c).wait_recv()
        total[c] = total[c] + acc_in[c].astype(jnp.float32)
        result_copy(c).start()
    for i in range(6):
        weight_copy(i).wait_send()
    for i in range(8):
        row_copy(i).wait_send()
    for i in range(1, experts):
        route_copy(i).wait_send()
    for c in range(CHUNKS):
        far_copy(c).wait_send()
        near_copy(c).wait_send()
        sum_copy(c).wait_send()
        result_copy(c).wait()


STEP_ROWS = 64


def update(
    grad_hbm,
    anchor_ref,
    average_ref,
    moment_hbm,
    anchor_out,
    average_out,
    moment_out,
    grad_ref,
    moment_ref,
    held,
    in_sem,
    sem,
):
    size = held.shape[2]
    steps = anchor_ref.shape[0] // size
    chunk = grad_hbm.shape[2]
    bias_two = 1.0 - beta_two**step_count

    def in_copy(k, i):
        at = pl.ds(pl.multiple_of(i * size, size), size)
        if k == 0:
            return pltpu.make_async_copy(grad_hbm.at[0:CHUNKS, at], grad_ref.at[i], in_sem.at[0, i])
        return pltpu.make_async_copy(moment_hbm.at[at], moment_ref.at[i], in_sem.at[1, i])

    def out_copy(k, i):
        at = pl.ds(pl.multiple_of(i * size, size), size)
        out = (anchor_out, average_out, moment_out)[k]
        return pltpu.make_async_copy(held.at[k, i % 2], out.at[at], sem.at[k, i % 2])

    for i in range(steps):
        for k in range(2):
            in_copy(k, i).start()

    def step(i, carry):
        @pl.when(i >= 2)
        def _():
            for k in range(3):
                out_copy(k, i - 2).wait()

        at = pl.ds(pl.multiple_of(i * size, size), size)
        slot = i % 2
        for k in range(2):
            in_copy(k, i).wait()
        for c in range(CHUNKS):
            cols = slice(c * chunk, (c + 1) * chunk)
            gradient = grad_ref[i, c] * FF ** (-0.5)
            anchor, average = anchor_ref[at, cols], average_ref[at, cols]
            moment = beta_two * moment_ref[i, :, cols] + (1.0 - beta_two) * (gradient * gradient)
            square = moment * (1.0 / bias_two)
            root = square * lax.rsqrt(square)
            kept = (1.0 - learn_rate * decay_rate * (1.0 - beta_one)) * anchor - (
                learn_rate * decay_rate * beta_one
            ) * average
            new_anchor = kept - (learn_rate * gradient) / (root + epsilon)
            held[0, slot, :, cols] = new_anchor
            held[1, slot, :, cols] = (
                1.0 - 1.0 / step_count
            ) * average + 1.0 / step_count * new_anchor
            held[2, slot, :, cols] = moment
        for k in range(3):
            out_copy(k, i).start()
        return carry

    lax.fori_loop(0, steps, step, 0)
    for i in range(max(steps - 2, 0), steps):
        for k in range(3):
            out_copy(k, i).wait()


def shards(
    tokens,
    cotangent,
    expert_ids,
    route_share,
    gate_proj,
    up_proj,
    down_anchor,
    down_average,
    down_moment,
):
    experts = lax.axis_size("expert")
    toks, width = tokens.shape
    cap = toks * TOPK // experts * 9 // 8
    block = experts * cap
    full = gate_proj.shape[1]
    chunk = width // CHUNKS
    bf16 = jnp.bfloat16
    vmem = pl.BlockSpec(memory_space=pltpu.VMEM)
    hbm = pl.BlockSpec(memory_space=pl.ANY)
    dma = pltpu.SemaphoreType.DMA
    gradient = pl.pallas_call(
        functools.partial(exchange, experts, cap),
        out_shape=jax.ShapeDtypeStruct((6 * CHUNKS, full, chunk), jnp.float32),
        in_specs=[vmem, vmem, vmem, vmem, hbm, hbm],
        out_specs=hbm,
        scratch_shapes=[
            pltpu.VMEM((experts, 2 * cap, width), bf16),
            pltpu.VMEM((experts, 2 * cap, width), bf16),
            pltpu.VMEM((SIDE, block, width), bf16),
            pltpu.VMEM((SIDE, block, width), bf16),
            pltpu.VMEM((SIDE, 2, full, width), bf16),
            pltpu.VMEM((SIDE, SIDE, block, full), bf16),
            pltpu.VMEM((full, SIDE * block), bf16),
            pltpu.VMEM((SIDE - 1, CHUNKS, full, chunk), bf16),
            pltpu.VMEM((CHUNKS, full, chunk), bf16),
            pltpu.VMEM((CHUNKS, full, chunk), bf16),
            pltpu.VMEM((CHUNKS, full, chunk), bf16),
            pltpu.VMEM((CHUNKS, full, chunk), jnp.float32),
            dma((2 + CHUNKS,)),
            dma((6,)),
            dma((6,)),
            dma((experts - 1,)),
            dma((experts - 1,)),
            dma((8,)),
            dma((8,)),
            dma((CHUNKS,)),
            dma((CHUNKS,)),
            dma((CHUNKS,)),
            dma((CHUNKS,)),
            dma((CHUNKS,)),
            dma((CHUNKS,)),
        ],
        compiler_params=pltpu.CompilerParams(
            collective_id=0, has_side_effects=True, vmem_limit_bytes=54 * 1024 * 1024
        ),
        name="exchange",
    )(tokens, cotangent, expert_ids.T, route_share[None], gate_proj[0], up_proj[0])
    size = STEP_ROWS if full % STEP_ROWS == 0 else full
    whole = jax.ShapeDtypeStruct((full, width), jnp.float32)
    outs = pl.pallas_call(
        update,
        out_shape=(whole, whole, whole),
        in_specs=[hbm, vmem, vmem, hbm],
        out_specs=(hbm, hbm, hbm),
        scratch_shapes=[
            pltpu.VMEM((full // size, CHUNKS, size, chunk), jnp.float32),
            pltpu.VMEM((full // size, size, width), jnp.float32),
            pltpu.VMEM((3, 2, size, width), jnp.float32),
            dma((2, full // size)),
            dma((3, 2)),
        ],
        compiler_params=pltpu.CompilerParams(vmem_limit_bytes=44 * 1024 * 1024),
        name="update",
    )(gradient, down_anchor[0], down_average[0], down_moment[0])
    return tuple(out[None] for out in outs)


def solution(mesh):
    placed = (
        P(("dp", "expert"), None),
        P(("dp", "expert"), None),
        P(("dp", "expert"), None),
        P(("dp", "expert")),
        P("expert", "dp", None),
        P("expert", "dp", None),
        P("expert", "dp", None),
        P("expert", "dp", None),
        P("expert", "dp", None),
    )
    return jax.shard_map(
        shards,
        mesh=mesh,
        in_specs=placed,
        out_specs=(P("expert", "dp", None), P("expert", "dp", None), P("expert", "dp", None)),
        check_vma=False,
    )
```

```python
import functools

import jax
import jax.numpy as jnp
from jax import lax
from jax.experimental import pallas as pl
from jax.experimental.pallas import tpu as pltpu
from jax.sharding import PartitionSpec as P

FF = 7168
TOPK = 2

beta_one = 0.9
beta_two = 0.95
learn_rate = 0.05
decay_rate = 0.1
step_count = 4.0
epsilon = 1e-08

SIDE = 4
CHUNKS = 4
MESH = pl.DeviceIdType.MESH
NT = (((1,), (1,)), ((), ()))


def dot(a, b):
    return jnp.dot(a, b, preferred_element_type=jnp.float32)


def exchange(
    experts,
    cap,
    tok_hbm,
    cot_hbm,
    ids_hbm,
    share_hbm,
    gate_ref,
    up_ref,
    out_ref,
    tok_ref,
    cot_ref,
    ids_ref,
    share_ref,
    pack,
    land,
    rows,
    grads,
    weights,
    hid,
    hid_t,
    part,
    opp_in,
    dir_in,
    acc_in,
    total,
    own_sem,
    w_send,
    w_recv,
    a_send,
    a_recv,
    r_send,
    r_recv,
    opp_send,
    opp_recv,
    dir_send,
    dir_recv,
    acc_send,
    acc_recv,
):
    dp = lax.axis_index("dp")
    me = lax.axis_index("expert")
    core = me % 2
    hi, lo = dp // SIDE, dp % SIDE
    p = core * hi + (1 - core) * lo
    q = core * lo + (1 - core) * hi

    def peer(p_to, q_to, e_to):
        to = core * (p_to * SIDE + q_to) + (1 - core) * (q_to * SIDE + p_to)
        return {"dp": to, "expert": e_to}

    p_left, p_right, p_far = (p + 3) % SIDE, (p + 1) % SIDE, (p + 2) % SIDE
    q_left, q_right, q_far = (q + 3) % SIDE, (q + 1) % SIDE, (q + 2) % SIDE
    w_left, w_right = peer(p_left, q, me), peer(p_right, q, me)
    r_left, r_right = peer(p, q_left, me), peer(p, q_right, me)

    barrier = pltpu.get_barrier_semaphore()
    for to in (w_left, w_right, r_left, r_right):
        pl.semaphore_signal(barrier, inc=1, device_id=to, device_id_type=MESH)
    for i in range(1, experts):
        pl.semaphore_signal(
            barrier, inc=1, device_id=peer(p, q, (me + i) % experts), device_id_type=MESH
        )

    def remote(src, dst, send, recv, to):
        return pltpu.make_async_remote_copy(
            src_ref=src, dst_ref=dst, send_sem=send, recv_sem=recv, device_id=to,
            device_id_type=MESH,
        )

    def weight_copy(i):
        if i == 0:
            return remote(gate_ref, weights.at[p, 0], w_send.at[0], w_recv.at[0], w_left)
        if i == 1:
            return remote(up_ref, weights.at[p, 1], w_send.at[1], w_recv.at[1], w_right)
        if i == 2:
            return remote(up_ref, weights.at[p, 1], w_send.at[2], w_recv.at[2], w_left)
        if i == 3:
            return remote(gate_ref, weights.at[p, 0], w_send.at[3], w_recv.at[3], w_right)
        if i == 4:
            ref = weights.at[p_right, 0]
            return remote(ref, ref, w_send.at[4], w_recv.at[4], w_left)
        ref = weights.at[p_left, 1]
        return remote(ref, ref, w_send.at[5], w_recv.at[5], w_right)

    own_gate = pltpu.make_async_copy(gate_ref, weights.at[p, 0], own_sem.at[0])
    own_up = pltpu.make_async_copy(up_ref, weights.at[p, 1], own_sem.at[1])
    inputs = [
        pltpu.make_async_copy(src, dst, own_sem.at[2 + CHUNKS + i])
        for i, (src, dst) in enumerate(
            (
                (ids_hbm, ids_ref),
                (share_hbm, share_ref),
                (tok_hbm, tok_ref),
                (cot_hbm, cot_ref),
            )
        )
    ]
    for copy in inputs:
        copy.start()

    pl.semaphore_wait(barrier, 4 + experts - 1)
    for i in range(4):
        weight_copy(i).start()
    own_gate.start()
    own_up.start()
    for copy in inputs:
        copy.wait()

    toks = tok_ref.shape[0]
    number = lax.broadcasted_iota(jnp.int32, (experts, toks), 0)
    before = (
        lax.broadcasted_iota(jnp.int32, (toks, toks), 0)
        < lax.broadcasted_iota(jnp.int32, (toks, toks), 1)
    ).astype(jnp.bfloat16)
    id_a, id_b = ids_ref[0:1, :], ids_ref[1:2, :]
    hot_a = (number == id_a).astype(jnp.float32)
    hot_b = (number == id_b).astype(jnp.float32)
    count_a = dot(hot_a.astype(jnp.bfloat16), before)
    count_b = dot(hot_b.astype(jnp.bfloat16), before) + jnp.sum(hot_a, axis=1, keepdims=True)
    slot_a = jnp.sum(hot_a * count_a, axis=0, keepdims=True).astype(jnp.int32)
    slot_b = jnp.sum(hot_b * count_b, axis=0, keepdims=True).astype(jnp.int32)
    share = share_ref[...]
    line = lax.broadcasted_iota(jnp.int32, (2 * cap, toks), 0)

    def fill(i, carry):
        to = (me + i) % experts
        at_a = jnp.where(id_a == to, slot_a, -1 - 2 * cap)
        at_b = jnp.where(id_b == to, slot_b, -1 - 2 * cap)
        row_pick = ((line == at_a) | (line == at_b)).astype(jnp.float32).astype(jnp.bfloat16)
        low_a, low_b = line == at_a + cap, line == at_b + cap
        grad_pick = (low_a | low_b).astype(jnp.float32).astype(jnp.bfloat16)
        scale = jnp.sum(
            jnp.where(low_a, share, 0.0) + jnp.where(low_b, 1.0 - share, 0.0),
            axis=1,
            keepdims=True,
        )
        both = dot(row_pick, tok_ref[...]) + scale * dot(grad_pick, cot_ref[...])
        pack[to] = both.astype(jnp.bfloat16)
        return carry

    lax.fori_loop(0, experts, fill, 0)

    def route_copy(i):
        to = (me + i) % experts
        return remote(
            pack.at[to], land.at[me], a_send.at[i - 1], a_recv.at[i - 1], peer(p, q, to)
        )

    for i in range(1, experts):
        route_copy(i).start()
    land[me] = pack[me]

    for i in range(1, experts):
        route_copy(i).wait_recv()

    block = experts * cap
    wide = lax.broadcasted_iota(jnp.int32, (block, 2 * block), 1)
    deep = lax.broadcasted_iota(jnp.int32, (block, 2 * block), 0)
    source = jnp.floor((wide.astype(jnp.float32) + 0.5) * (1.0 / (2 * cap))).astype(jnp.int32)
    inside = wide - source * (2 * cap)
    row_from = jnp.where(inside < cap, source * cap + inside, -1)
    grad_from = jnp.where(inside >= cap, source * cap + inside - cap, -1)
    landed = land[...].reshape(2 * block, land.shape[2])
    pick = (deep == row_from).astype(jnp.float32).astype(jnp.bfloat16)
    rows[q] = dot(pick, landed).astype(jnp.bfloat16)
    pick = (deep == grad_from).astype(jnp.float32).astype(jnp.bfloat16)
    grads[q] = dot(pick, landed).astype(jnp.bfloat16)

    def row_copy(i):
        if i == 0:
            return remote(rows.at[q], rows.at[q], r_send.at[0], r_recv.at[0], r_left)
        if i == 1:
            return remote(grads.at[q], grads.at[q], r_send.at[1], r_recv.at[1], r_right)
        if i == 2:
            return remote(grads.at[q], grads.at[q], r_send.at[2], r_recv.at[2], r_left)
        if i == 3:
            return remote(rows.at[q], rows.at[q], r_send.at[3], r_recv.at[3], r_right)
        half = pl.ds((i - 4) // 2 * (block // 2), block // 2)
        if i % 2 == 0:
            ref = rows.at[q_right, half]
            return remote(ref, ref, r_send.at[i], r_recv.at[i], r_left)
        ref = grads.at[q_left, half]
        return remote(ref, ref, r_send.at[i], r_recv.at[i], r_right)

    for i in range(4):
        row_copy(i).start()

    def forward(b, s, slot):
        x = rows[b]
        gate = lax.dot_general(x, weights[s, 0], NT, preferred_element_type=jnp.float32)
        up = lax.dot_general(x, weights[s, 1], NT, preferred_element_type=jnp.float32)
        hid[slot, b] = (gate / (1.0 + jnp.exp(-gate)) * up).astype(jnp.bfloat16)

    def forward_near(b):
        def step(i, carry):
            forward(b, (p + 3 + i) % SIDE, i)
            return carry

        lax.fori_loop(0, 3, step, 0)

    own_gate.wait()
    own_up.wait()
    for i in range(4):
        weight_copy(i).wait_recv()
    forward_near(q)
    row_copy(0).wait_recv()
    row_copy(4).start()
    row_copy(6).start()
    row_copy(1).wait_recv()
    row_copy(5).start()
    row_copy(7).start()
    forward_near(q_right)
    row_copy(3).wait_recv()
    forward_near(q_left)
    row_copy(2).wait_recv()
    row_copy(4).wait_recv()
    weight_copy(4).start()
    row_copy(5).wait_recv()
    weight_copy(5).start()
    row_copy(6).wait_recv()
    row_copy(7).wait_recv()

    def far_copy(c):
        return remote(
            part.at[1, c], opp_in.at[c], opp_send.at[c], opp_recv.at[c],
            peer((p + 3 + 2 * (c // 2)) % SIDE, q, me),
        )

    def near_copy(c):
        to = (p + 1 + 2 * (c // 2)) % SIDE
        return remote(
            part.at[2 * (c // 2), c], dir_in.at[c], dir_send.at[c], dir_recv.at[c], peer(to, q, me)
        )

    def sum_copy(c):
        to = (p + 3 + 2 * (c // 2)) % SIDE
        return remote(
            part.at[2 - 2 * (c // 2), c], acc_in.at[c], acc_send.at[c], acc_recv.at[c], peer(to, q, me)
        )

    all_rows = SIDE * block
    full = hid.shape[3]
    chunk = part.shape[3]

    def turn(slot):
        hid_t[...] = hid[slot].reshape(all_rows, full).T

    def backward(c):
        at = pl.ds(pl.multiple_of(c * chunk, chunk), chunk)
        return dot(hid_t[...], grads[:, :, at].reshape(all_rows, chunk))

    def near_slice(first, s, place, slot):
        forward(q_far, s, slot)
        turn(slot)

        def step(j, carry):
            c = (first + j) % CHUNKS
            part[place, c] = backward(c).astype(jnp.bfloat16)

            @pl.when(j < 2)
            def _():
                near_copy(c).start()

            return carry

        lax.fori_loop(0, CHUNKS, step, 0)

    near_slice(2, p_left, 2, 0)
    near_slice(0, p_right, 0, 2)
    forward(q_far, p, 1)
    turn(1)

    def own_step(c, carry):
        total[c] = backward(c)
        return carry

    lax.fori_loop(0, CHUNKS, own_step, 0)

    weight_copy(4).wait_recv()
    weight_copy(5).wait_recv()

    def far_forward(b, carry):
        forward(b, p_far, 0)
        return carry

    lax.fori_loop(0, SIDE, far_forward, 0)
    turn(0)

    def far_step(j, carry):
        c = (j % 2) * 2 + j // 2
        part[1, c] = backward(c).astype(jnp.bfloat16)
        far_copy(c).start()
        return carry

    lax.fori_loop(0, CHUNKS, far_step, 0)

    def relay(j, carry):
        c = (j % 2) * 2 + j // 2
        far_copy(c).wait_recv()
        place = 2 - 2 * (c // 2)
        part[place, c] = (
            part[place, c].astype(jnp.float32) + opp_in[c].astype(jnp.float32)
        ).astype(jnp.bfloat16)
        sum_copy(c).start()
        return carry

    lax.fori_loop(0, CHUNKS, relay, 0)

    def result_copy(c):
        return pltpu.make_async_copy(total.at[c], out_ref.at[c], own_sem.at[2 + c])

    for c in range(CHUNKS):
        near_copy(c).wait_recv()
        total[c] = total[c] + dir_in[c].astype(jnp.float32)
    for c in (0, 2, 1, 3):
        sum_copy(c).wait_recv()
        total[c] = total[c] + acc_in[c].astype(jnp.float32)
        result_copy(c).start()
    for i in range(6):
        weight_copy(i).wait_send()
    for i in range(8):
        row_copy(i).wait_send()
    for i in range(1, experts):
        route_copy(i).wait_send()
    for c in range(CHUNKS):
        far_copy(c).wait_send()
        near_copy(c).wait_send()
        sum_copy(c).wait_send()
        result_copy(c).wait()


STEP_ROWS = 64


def update(
    grad_hbm,
    anchor_ref,
    average_ref,
    moment_hbm,
    anchor_out,
    average_out,
    moment_out,
    grad_ref,
    moment_ref,
    held,
    in_sem,
    sem,
):
    size = held.shape[2]
    steps = anchor_ref.shape[0] // size
    chunk = grad_hbm.shape[2]
    bias_two = 1.0 - beta_two**step_count

    def in_copy(k, i):
        at = pl.ds(pl.multiple_of(i * size, size), size)
        if k == 0:
            return pltpu.make_async_copy(grad_hbm.at[0:CHUNKS, at], grad_ref.at[i], in_sem.at[0, i])
        return pltpu.make_async_copy(moment_hbm.at[at], moment_ref.at[i], in_sem.at[1, i])

    def out_copy(k, i):
        at = pl.ds(pl.multiple_of(i * size, size), size)
        out = (anchor_out, average_out, moment_out)[k]
        return pltpu.make_async_copy(held.at[k, i], out.at[at], sem.at[k, i])

    for i in range(steps):
        for k in range(2):
            in_copy(k, i).start()

    def step(i, carry):
        at = pl.ds(pl.multiple_of(i * size, size), size)
        for k in range(2):
            in_copy(k, i).wait()
        for c in range(CHUNKS):
            cols = slice(c * chunk, (c + 1) * chunk)
            gradient = grad_ref[i, c] * FF ** (-0.5)
            anchor, average = anchor_ref[at, cols], average_ref[at, cols]
            moment = beta_two * moment_ref[i, :, cols] + (1.0 - beta_two) * (gradient * gradient)
            square = moment * (1.0 / bias_two)
            root = square * lax.rsqrt(square)
            kept = (1.0 - learn_rate * decay_rate * (1.0 - beta_one)) * anchor - (
                learn_rate * decay_rate * beta_one
            ) * average
            new_anchor = kept - (learn_rate * gradient) / (root + epsilon)
            held[0, i, :, cols] = new_anchor
            held[1, i, :, cols] = (
                1.0 - 1.0 / step_count
            ) * average + 1.0 / step_count * new_anchor
            held[2, i, :, cols] = moment
        for k in range(3):
            out_copy(k, i).start()
        return carry

    lax.fori_loop(0, steps, step, 0)
    for i in range(steps):
        for k in range(3):
            out_copy(k, i).wait()


def shards(
    tokens,
    cotangent,
    expert_ids,
    route_share,
    gate_proj,
    up_proj,
    down_anchor,
    down_average,
    down_moment,
):
    experts = lax.axis_size("expert")
    toks, width = tokens.shape
    cap = toks * TOPK // experts * 9 // 8
    block = experts * cap
    full = gate_proj.shape[1]
    chunk = width // CHUNKS
    bf16 = jnp.bfloat16
    vmem = pl.BlockSpec(memory_space=pltpu.VMEM)
    hbm = pl.BlockSpec(memory_space=pl.ANY)
    dma = pltpu.SemaphoreType.DMA
    gradient = pl.pallas_call(
        functools.partial(exchange, experts, cap),
        out_shape=jax.ShapeDtypeStruct((6 * CHUNKS, full, chunk), jnp.float32),
        in_specs=[hbm] * 6,
        out_specs=hbm,
        scratch_shapes=[
            pltpu.VMEM((toks, width), bf16),
            pltpu.VMEM((toks, width), bf16),
            pltpu.VMEM((TOPK, toks), jnp.int32),
            pltpu.VMEM((1, toks), jnp.float32),
            pltpu.VMEM((experts, 2 * cap, width), bf16),
            pltpu.VMEM((experts, 2 * cap, width), bf16),
            pltpu.VMEM((SIDE, block, width), bf16),
            pltpu.VMEM((SIDE, block, width), bf16),
            pltpu.VMEM((SIDE, 2, full, width), bf16),
            pltpu.VMEM((SIDE - 1, SIDE, block, full), bf16),
            pltpu.VMEM((full, SIDE * block), bf16),
            pltpu.VMEM((SIDE - 1, CHUNKS, full, chunk), bf16),
            pltpu.VMEM((CHUNKS, full, chunk), bf16),
            pltpu.VMEM((CHUNKS, full, chunk), bf16),
            pltpu.VMEM((CHUNKS, full, chunk), bf16),
            pltpu.VMEM((CHUNKS, full, chunk), jnp.float32),
            dma((6 + CHUNKS,)),
            dma((6,)),
            dma((6,)),
            dma((experts - 1,)),
            dma((experts - 1,)),
            dma((8,)),
            dma((8,)),
            dma((CHUNKS,)),
            dma((CHUNKS,)),
            dma((CHUNKS,)),
            dma((CHUNKS,)),
            dma((CHUNKS,)),
            dma((CHUNKS,)),
        ],
        compiler_params=pltpu.CompilerParams(
            collective_id=0, has_side_effects=True, vmem_limit_bytes=54 * 1024 * 1024
        ),
        name="exchange",
    )(tokens, cotangent, expert_ids.T, route_share[None], gate_proj[0], up_proj[0])
    size = STEP_ROWS if full % STEP_ROWS == 0 else full
    whole = jax.ShapeDtypeStruct((full, width), jnp.float32)
    outs = pl.pallas_call(
        update,
        out_shape=(whole, whole, whole),
        in_specs=[hbm, vmem, vmem, hbm],
        out_specs=(hbm, hbm, hbm),
        scratch_shapes=[
            pltpu.VMEM((full // size, CHUNKS, size, chunk), jnp.float32),
            pltpu.VMEM((full // size, size, width), jnp.float32),
            pltpu.VMEM((3, full // size, size, width), jnp.float32),
            dma((2, full // size)),
            dma((3, full // size)),
        ],
        compiler_params=pltpu.CompilerParams(vmem_limit_bytes=44 * 1024 * 1024),
        name="update",
    )(gradient, down_anchor[0], down_average[0], down_moment[0])
    return tuple(out[None] for out in outs)


def solution(mesh):
    placed = (
        P(("dp", "expert"), None),
        P(("dp", "expert"), None),
        P(("dp", "expert"), None),
        P(("dp", "expert")),
        P("expert", "dp", None),
        P("expert", "dp", None),
        P("expert", "dp", None),
        P("expert", "dp", None),
        P("expert", "dp", None),
    )
    return jax.shard_map(
        shards,
        mesh=mesh,
        in_specs=placed,
        out_specs=(P("expert", "dp", None), P("expert", "dp", None), P("expert", "dp", None)),
        check_vma=False,
    )
```

```python
import functools

import jax
import jax.numpy as jnp
from jax import lax
from jax.experimental import pallas as pl
from jax.experimental.pallas import tpu as pltpu
from jax.sharding import PartitionSpec as P

FF = 7168
TOPK = 2

beta_one = 0.9
beta_two = 0.95
learn_rate = 0.05
decay_rate = 0.1
step_count = 4.0
epsilon = 1e-08

SIDE = 4
CHUNKS = 4
MESH = pl.DeviceIdType.MESH
NT = (((1,), (1,)), ((), ()))


def dot(a, b):
    return jnp.dot(a, b, preferred_element_type=jnp.float32)


def exchange(
    experts,
    cap,
    tok_hbm,
    cot_hbm,
    ids_hbm,
    share_hbm,
    gate_ref,
    up_ref,
    out_ref,
    tok_ref,
    cot_ref,
    ids_ref,
    share_ref,
    pack,
    land,
    rows,
    grads,
    weights,
    hid,
    hid_t,
    part,
    opp_in,
    dir_in,
    acc_in,
    total,
    own_sem,
    w_send,
    w_recv,
    a_send,
    a_recv,
    r_send,
    r_recv,
    opp_send,
    opp_recv,
    dir_send,
    dir_recv,
    acc_send,
    acc_recv,
):
    dp = lax.axis_index("dp")
    me = lax.axis_index("expert")
    core = me % 2
    hi, lo = dp // SIDE, dp % SIDE
    p = core * hi + (1 - core) * lo
    q = core * lo + (1 - core) * hi

    def peer(p_to, q_to, e_to):
        to = core * (p_to * SIDE + q_to) + (1 - core) * (q_to * SIDE + p_to)
        return {"dp": to, "expert": e_to}

    p_left, p_right, p_far = (p + 3) % SIDE, (p + 1) % SIDE, (p + 2) % SIDE
    q_left, q_right, q_far = (q + 3) % SIDE, (q + 1) % SIDE, (q + 2) % SIDE
    w_left, w_right = peer(p_left, q, me), peer(p_right, q, me)
    r_left, r_right = peer(p, q_left, me), peer(p, q_right, me)

    barrier = pltpu.get_barrier_semaphore()
    for to in (w_left, w_right, r_left, r_right):
        pl.semaphore_signal(barrier, inc=1, device_id=to, device_id_type=MESH)
    for i in range(1, experts):
        pl.semaphore_signal(
            barrier, inc=1, device_id=peer(p, q, (me + i) % experts), device_id_type=MESH
        )

    def remote(src, dst, send, recv, to):
        return pltpu.make_async_remote_copy(
            src_ref=src, dst_ref=dst, send_sem=send, recv_sem=recv, device_id=to,
            device_id_type=MESH,
        )

    def weight_copy(i):
        if i == 0:
            return remote(gate_ref, weights.at[p, 0], w_send.at[0], w_recv.at[0], w_left)
        if i == 1:
            return remote(up_ref, weights.at[p, 1], w_send.at[1], w_recv.at[1], w_right)
        if i == 2:
            return remote(up_ref, weights.at[p, 1], w_send.at[2], w_recv.at[2], w_left)
        if i == 3:
            return remote(gate_ref, weights.at[p, 0], w_send.at[3], w_recv.at[3], w_right)
        if i == 4:
            ref = weights.at[p_right, 0]
            return remote(ref, ref, w_send.at[4], w_recv.at[4], w_left)
        ref = weights.at[p_left, 1]
        return remote(ref, ref, w_send.at[5], w_recv.at[5], w_right)

    own_gate = pltpu.make_async_copy(gate_ref, weights.at[p, 0], own_sem.at[0])
    own_up = pltpu.make_async_copy(up_ref, weights.at[p, 1], own_sem.at[1])
    inputs = [
        pltpu.make_async_copy(src, dst, own_sem.at[2 + CHUNKS + i])
        for i, (src, dst) in enumerate(
            (
                (ids_hbm, ids_ref),
                (share_hbm, share_ref),
                (tok_hbm, tok_ref),
                (cot_hbm, cot_ref),
            )
        )
    ]
    for copy in inputs:
        copy.start()

    pl.semaphore_wait(barrier, 4 + experts - 1)
    for i in range(4):
        weight_copy(i).start()
    own_gate.start()
    own_up.start()
    for copy in inputs:
        copy.wait()

    toks = tok_ref.shape[0]
    number = lax.broadcasted_iota(jnp.int32, (experts, toks), 0)
    before = (
        lax.broadcasted_iota(jnp.int32, (toks, toks), 0)
        < lax.broadcasted_iota(jnp.int32, (toks, toks), 1)
    ).astype(jnp.bfloat16)
    id_a, id_b = ids_ref[0:1, :], ids_ref[1:2, :]
    hot_a = (number == id_a).astype(jnp.float32)
    hot_b = (number == id_b).astype(jnp.float32)
    count_a = dot(hot_a.astype(jnp.bfloat16), before)
    count_b = dot(hot_b.astype(jnp.bfloat16), before) + jnp.sum(hot_a, axis=1, keepdims=True)
    slot_a = jnp.sum(hot_a * count_a, axis=0, keepdims=True).astype(jnp.int32)
    slot_b = jnp.sum(hot_b * count_b, axis=0, keepdims=True).astype(jnp.int32)
    share = share_ref[...]
    line = lax.broadcasted_iota(jnp.int32, (2 * cap, toks), 0)

    def fill(i, carry):
        to = (me + i) % experts
        at_a = jnp.where(id_a == to, slot_a, -1 - 2 * cap)
        at_b = jnp.where(id_b == to, slot_b, -1 - 2 * cap)
        row_pick = ((line == at_a) | (line == at_b)).astype(jnp.float32).astype(jnp.bfloat16)
        low_a, low_b = line == at_a + cap, line == at_b + cap
        grad_pick = (low_a | low_b).astype(jnp.float32).astype(jnp.bfloat16)
        scale = jnp.sum(
            jnp.where(low_a, share, 0.0) + jnp.where(low_b, 1.0 - share, 0.0),
            axis=1,
            keepdims=True,
        )
        both = dot(row_pick, tok_ref[...]) + scale * dot(grad_pick, cot_ref[...])
        pack[to] = both.astype(jnp.bfloat16)
        return carry

    lax.fori_loop(0, experts, fill, 0)

    def route_copy(i):
        to = (me + i) % experts
        return remote(
            pack.at[to], land.at[me], a_send.at[i - 1], a_recv.at[i - 1], peer(p, q, to)
        )

    for i in range(1, experts):
        route_copy(i).start()
    land[me] = pack[me]

    for i in range(1, experts):
        route_copy(i).wait_recv()

    block = experts * cap
    wide = lax.broadcasted_iota(jnp.int32, (block, 2 * block), 1)
    deep = lax.broadcasted_iota(jnp.int32, (block, 2 * block), 0)
    source = jnp.floor((wide.astype(jnp.float32) + 0.5) * (1.0 / (2 * cap))).astype(jnp.int32)
    inside = wide - source * (2 * cap)
    row_from = jnp.where(inside < cap, source * cap + inside, -1)
    grad_from = jnp.where(inside >= cap, source * cap + inside - cap, -1)
    landed = land[...].reshape(2 * block, land.shape[2])
    pick = (deep == row_from).astype(jnp.float32).astype(jnp.bfloat16)
    rows[q] = dot(pick, landed).astype(jnp.bfloat16)
    pick = (deep == grad_from).astype(jnp.float32).astype(jnp.bfloat16)
    grads[q] = dot(pick, landed).astype(jnp.bfloat16)

    def row_copy(i):
        if i == 0:
            return remote(rows.at[q], rows.at[q], r_send.at[0], r_recv.at[0], r_left)
        if i == 1:
            return remote(grads.at[q], grads.at[q], r_send.at[1], r_recv.at[1], r_right)
        if i == 2:
            return remote(grads.at[q], grads.at[q], r_send.at[2], r_recv.at[2], r_left)
        if i == 3:
            return remote(rows.at[q], rows.at[q], r_send.at[3], r_recv.at[3], r_right)
        half = pl.ds((i - 4) // 2 * (block // 2), block // 2)
        if i % 2 == 0:
            ref = rows.at[q_right, half]
            return remote(ref, ref, r_send.at[i], r_recv.at[i], r_left)
        ref = grads.at[q_left, half]
        return remote(ref, ref, r_send.at[i], r_recv.at[i], r_right)

    for i in range(4):
        row_copy(i).start()

    def forward(b, s, slot):
        x = rows[b]
        gate = lax.dot_general(x, weights[s, 0], NT, preferred_element_type=jnp.float32)
        up = lax.dot_general(x, weights[s, 1], NT, preferred_element_type=jnp.float32)
        hid[slot, b] = (gate / (1.0 + jnp.exp(-gate)) * up).astype(jnp.bfloat16)

    def forward_near(b):
        def step(i, carry):
            forward(b, (p + 3 + i) % SIDE, i)
            return carry

        lax.fori_loop(0, 3, step, 0)

    own_gate.wait()
    own_up.wait()
    for i in range(4):
        weight_copy(i).wait_recv()
    forward_near(q)
    row_copy(0).wait_recv()
    row_copy(4).start()
    row_copy(6).start()
    row_copy(1).wait_recv()
    row_copy(5).start()
    row_copy(7).start()
    forward_near(q_right)
    row_copy(3).wait_recv()
    forward_near(q_left)
    row_copy(2).wait_recv()
    row_copy(4).wait_recv()
    weight_copy(4).start()
    row_copy(5).wait_recv()
    weight_copy(5).start()
    row_copy(6).wait_recv()
    row_copy(7).wait_recv()

    def far_copy(c):
        return remote(
            part.at[1, c], opp_in.at[c], opp_send.at[c], opp_recv.at[c],
            peer((p + 3 + 2 * (c // 2)) % SIDE, q, me),
        )

    def near_copy(c):
        to = (p + 1 + 2 * (c // 2)) % SIDE
        return remote(
            part.at[2 * (c // 2), c], dir_in.at[c], dir_send.at[c], dir_recv.at[c], peer(to, q, me)
        )

    def sum_copy(c):
        to = (p + 3 + 2 * (c // 2)) % SIDE
        return remote(
            part.at[2 - 2 * (c // 2), c], acc_in.at[c], acc_send.at[c], acc_recv.at[c], peer(to, q, me)
        )

    all_rows = SIDE * block
    full = hid.shape[3]
    chunk = part.shape[3]

    def turn(slot):
        hid_t[...] = hid[slot].reshape(all_rows, full).T

    def backward(c):
        at = pl.ds(pl.multiple_of(c * chunk, chunk), chunk)
        return dot(hid_t[...], grads[:, :, at].reshape(all_rows, chunk))

    def near_slice(first, s, place, slot):
        forward(q_far, s, slot)
        turn(slot)

        def step(j, carry):
            c = (first + j) % CHUNKS
            part[place, c] = backward(c).astype(jnp.bfloat16)

            @pl.when(j < 2)
            def _():
                near_copy(c).start()

            return carry

        lax.fori_loop(0, CHUNKS, step, 0)

    near_slice(2, p_left, 2, 0)
    near_slice(0, p_right, 0, 2)
    forward(q_far, p, 1)
    turn(1)

    def own_step(c, carry):
        total[c] = backward(c)
        return carry

    lax.fori_loop(0, CHUNKS, own_step, 0)

    weight_copy(4).wait_recv()
    weight_copy(5).wait_recv()

    def far_forward(b, carry):
        forward(b, p_far, 0)
        return carry

    lax.fori_loop(0, SIDE, far_forward, 0)
    turn(0)

    def far_step(j, carry):
        c = (j % 2) * 2 + j // 2
        part[1, c] = backward(c).astype(jnp.bfloat16)
        far_copy(c).start()
        return carry

    lax.fori_loop(0, CHUNKS, far_step, 0)

    def relay(j, carry):
        c = (j % 2) * 2 + j // 2
        far_copy(c).wait_recv()
        place = 2 - 2 * (c // 2)
        part[place, c] = (
            part[place, c].astype(jnp.float32) + opp_in[c].astype(jnp.float32)
        ).astype(jnp.bfloat16)
        sum_copy(c).start()
        return carry

    lax.fori_loop(0, CHUNKS, relay, 0)

    def result_copy(c):
        return pltpu.make_async_copy(total.at[c], out_ref.at[c], own_sem.at[2 + c])

    for c in range(CHUNKS):
        near_copy(c).wait_recv()
        total[c] = total[c] + dir_in[c].astype(jnp.float32)
    for c in (0, 2, 1, 3):
        sum_copy(c).wait_recv()
        total[c] = total[c] + acc_in[c].astype(jnp.float32)
        result_copy(c).start()
    for i in range(6):
        weight_copy(i).wait_send()
    for i in range(8):
        row_copy(i).wait_send()
    for i in range(1, experts):
        route_copy(i).wait_send()
    for c in range(CHUNKS):
        far_copy(c).wait_send()
        near_copy(c).wait_send()
        sum_copy(c).wait_send()
        result_copy(c).wait()


STEP_ROWS = 32


def update(
    grad_hbm,
    anchor_ref,
    average_ref,
    moment_hbm,
    anchor_out,
    average_out,
    moment_out,
    grad_ref,
    moment_ref,
    held,
    in_sem,
    sem,
):
    size = held.shape[2]
    steps = anchor_ref.shape[0] // size
    chunk = grad_hbm.shape[2]
    bias_two = 1.0 - beta_two**step_count

    def in_copy(k, i):
        at = pl.ds(pl.multiple_of(i * size, size), size)
        if k == 0:
            return pltpu.make_async_copy(grad_hbm.at[0:CHUNKS, at], grad_ref.at[i], in_sem.at[0, i])
        return pltpu.make_async_copy(moment_hbm.at[at], moment_ref.at[i], in_sem.at[1, i])

    def out_copy(k, i):
        at = pl.ds(pl.multiple_of(i * size, size), size)
        out = (anchor_out, average_out, moment_out)[k]
        return pltpu.make_async_copy(held.at[k, i], out.at[at], sem.at[k, i])

    for i in range(steps):
        for k in range(2):
            in_copy(k, i).start()

    def step(i, carry):
        at = pl.ds(pl.multiple_of(i * size, size), size)
        for k in range(2):
            in_copy(k, i).wait()
        for c in range(CHUNKS):
            cols = slice(c * chunk, (c + 1) * chunk)
            gradient = grad_ref[i, c] * FF ** (-0.5)
            anchor, average = anchor_ref[at, cols], average_ref[at, cols]
            moment = beta_two * moment_ref[i, :, cols] + (1.0 - beta_two) * (gradient * gradient)
            square = moment * (1.0 / bias_two)
            root = square * lax.rsqrt(square)
            kept = (1.0 - learn_rate * decay_rate * (1.0 - beta_one)) * anchor - (
                learn_rate * decay_rate * beta_one
            ) * average
            new_anchor = kept - (learn_rate * gradient) / (root + epsilon)
            held[0, i, :, cols] = new_anchor
            held[1, i, :, cols] = (
                1.0 - 1.0 / step_count
            ) * average + 1.0 / step_count * new_anchor
            held[2, i, :, cols] = moment
        for k in range(3):
            out_copy(k, i).start()
        return carry

    lax.fori_loop(0, steps, step, 0)
    for i in range(steps):
        for k in range(3):
            out_copy(k, i).wait()


def shards(
    tokens,
    cotangent,
    expert_ids,
    route_share,
    gate_proj,
    up_proj,
    down_anchor,
    down_average,
    down_moment,
):
    experts = lax.axis_size("expert")
    toks, width = tokens.shape
    cap = toks * TOPK // experts * 9 // 8
    block = experts * cap
    full = gate_proj.shape[1]
    chunk = width // CHUNKS
    bf16 = jnp.bfloat16
    vmem = pl.BlockSpec(memory_space=pltpu.VMEM)
    hbm = pl.BlockSpec(memory_space=pl.ANY)
    dma = pltpu.SemaphoreType.DMA
    gradient = pl.pallas_call(
        functools.partial(exchange, experts, cap),
        out_shape=jax.ShapeDtypeStruct((6 * CHUNKS, full, chunk), jnp.float32),
        in_specs=[hbm] * 6,
        out_specs=hbm,
        scratch_shapes=[
            pltpu.VMEM((toks, width), bf16),
            pltpu.VMEM((toks, width), bf16),
            pltpu.VMEM((TOPK, toks), jnp.int32),
            pltpu.VMEM((1, toks), jnp.float32),
            pltpu.VMEM((experts, 2 * cap, width), bf16),
            pltpu.VMEM((experts, 2 * cap, width), bf16),
            pltpu.VMEM((SIDE, block, width), bf16),
            pltpu.VMEM((SIDE, block, width), bf16),
            pltpu.VMEM((SIDE, 2, full, width), bf16),
            pltpu.VMEM((SIDE - 1, SIDE, block, full), bf16),
            pltpu.VMEM((full, SIDE * block), bf16),
            pltpu.VMEM((SIDE - 1, CHUNKS, full, chunk), bf16),
            pltpu.VMEM((CHUNKS, full, chunk), bf16),
            pltpu.VMEM((CHUNKS, full, chunk), bf16),
            pltpu.VMEM((CHUNKS, full, chunk), bf16),
            pltpu.VMEM((CHUNKS, full, chunk), jnp.float32),
            dma((6 + CHUNKS,)),
            dma((6,)),
            dma((6,)),
            dma((experts - 1,)),
            dma((experts - 1,)),
            dma((8,)),
            dma((8,)),
            dma((CHUNKS,)),
            dma((CHUNKS,)),
            dma((CHUNKS,)),
            dma((CHUNKS,)),
            dma((CHUNKS,)),
            dma((CHUNKS,)),
        ],
        compiler_params=pltpu.CompilerParams(
            collective_id=0, has_side_effects=True, vmem_limit_bytes=54 * 1024 * 1024
        ),
        name="exchange",
    )(tokens, cotangent, expert_ids.T, route_share[None], gate_proj[0], up_proj[0])
    size = STEP_ROWS if full % STEP_ROWS == 0 else full
    whole = jax.ShapeDtypeStruct((full, width), jnp.float32)
    outs = pl.pallas_call(
        update,
        out_shape=(whole, whole, whole),
        in_specs=[hbm, vmem, vmem, hbm],
        out_specs=(hbm, hbm, hbm),
        scratch_shapes=[
            pltpu.VMEM((full // size, CHUNKS, size, chunk), jnp.float32),
            pltpu.VMEM((full // size, size, width), jnp.float32),
            pltpu.VMEM((3, full // size, size, width), jnp.float32),
            dma((2, full // size)),
            dma((3, full // size)),
        ],
        compiler_params=pltpu.CompilerParams(vmem_limit_bytes=44 * 1024 * 1024),
        name="update",
    )(gradient, down_anchor[0], down_average[0], down_moment[0])
    return tuple(out[None] for out in outs)


def solution(mesh):
    placed = (
        P(("dp", "expert"), None),
        P(("dp", "expert"), None),
        P(("dp", "expert"), None),
        P(("dp", "expert")),
        P("expert", "dp", None),
        P("expert", "dp", None),
        P("expert", "dp", None),
        P("expert", "dp", None),
        P("expert", "dp", None),
    )
    return jax.shard_map(
        shards,
        mesh=mesh,
        in_specs=placed,
        out_specs=(P("expert", "dp", None), P("expert", "dp", None), P("expert", "dp", None)),
        check_vma=False,
    )
```
